32 devices in a mesh: ops: 8 (over z, x), sec: 4 (over y, core).
Axes of the slice: x: 2, y: 2, z: 4, core: 2. Of those that a mesh axis runs over, the one named last changes fastest.
Arguments:
- operators: bfloat16 [16, 8, 768, 768], P('ops', 'sec'), may hold values from -6 to 6
- basis: bfloat16 [8, 768, 768], P('sec'), may hold values from -0.21875 to 0.21875
- shift: int32 [16], replicated, may hold values from -1 to 1
- dest: int32 [16], replicated, may hold values from 0 to 15, each once
- sector_sizes: int32 [8], replicated, may hold values from 384 to 768
Outputs:
- renormalized: bfloat16 [16, 8, 768, 768], P('ops', 'sec')
The draws below stay inside these ranges and needn't reach their ends.
Inputs may be any that keep to these rules, and one draw needn't show every extreme that they name: `shift`: each pair's offset is -1, 0 or 1. dest names every index of 0 to 15 once.
All inputs are finite; a program needn't handle non-finite values.
Results may differ from the reference program's by a relative error of at most 0.0049.
Values may be sent and summed in bfloat16 or wider, within the bound.
A program may use at most 128 MiB of HBM per device.

```python
import jax
import jax.numpy as jnp
from jax import lax

M = 768
NSEC = 8
PAIRS = 16


def touch_ends(array, stream_key, smallest, largest):
    shape = array.shape
    index_at = [jax.random.randint(jax.random.fold_in(stream_key, axis), (), 0, shape[axis]) for axis in range(len(shape))]
    array = array.at[tuple(index_at)].set(smallest)
    longest = shape.index(max(shape))
    index_at[longest] = (index_at[longest] + 1) % shape[longest]
    return array.at[tuple(index_at)].set(largest)


def steps_of(own_key, dims, split, smallest, high):
    def one(dim, parts):
        draws = jax.random.uniform(jax.random.fold_in(jax.random.fold_in(own_key, 6), dim), (parts,), jnp.float32, smallest / len(split), high / len(split))
        return jnp.repeat(jnp.exp(draws), dims[dim] // parts).reshape((-1,) + (1,) * (len(dims) - dim - 1))

    level = one(*split[0])
    for cut in split[1:]:
        level = level * one(*cut)
    return level


def noise(own_key, dims, scale, limit, shards=(), held_as=jnp.bfloat16):
    result = jax.random.normal(own_key, dims, jnp.float32) * scale
    if len(shards) > 0:
        result = steps_of(own_key, dims, shards, -0.22, 0.18) * result
    return jnp.clip(result, min=-limit, max=limit).astype(held_as)


def setup_inputs(seed: int = 0) -> dict:
    splits = jax.random.split(jax.random.key(seed), 6)
    return {
        "operators": noise(splits[0], (PAIRS, NSEC, M, M), 1.0, 6.0, ((0, 8), (1, 4))),
        "basis": noise(splits[1], (NSEC, M, M), M ** -0.5, 0.21875, ((0, 4),)),
        "shift": touch_ends(jax.random.randint(splits[2], (PAIRS,), -1, 2), jax.random.fold_in(splits[2], 1), -1, 1).astype(jnp.int32),
        "dest": jax.random.permutation(splits[3], PAIRS).astype(jnp.int32),
        "sector_sizes": touch_ends(jax.random.randint(splits[4], (NSEC,), M // 2, M + 1), jax.random.fold_in(splits[4], 1), M // 2, M).astype(jnp.int32),
    }


def reference(operators, basis, shift, dest, sector_sizes):
    columns = jnp.arange(M, dtype=jnp.int32)
    kept = columns[None, :] < sector_sizes[:, None]
    kept_basis = jnp.where(kept[:, None, :], basis, jnp.zeros_like(basis))
    sector_ids = jnp.arange(NSEC, dtype=jnp.int32)

    def rotate_pair(packed):
        blocks, offset = packed
        target = (sector_ids + offset) % NSEC

        def one_sector(index):
            block = lax.dynamic_index_in_dim(blocks, index, 0, False)
            own = lax.dynamic_index_in_dim(kept_basis, index, 0, False)
            other = lax.dynamic_index_in_dim(kept_basis, target[index], 0, False)
            half = jnp.dot(block, own, preferred_element_type=jnp.float32).astype(jnp.bfloat16)
            return jnp.dot(other.T, half, preferred_element_type=jnp.float32).astype(jnp.bfloat16)

        return lax.map(one_sector, sector_ids)

    rotated = lax.map(rotate_pair, (operators, shift))
    source = jnp.zeros((PAIRS,), jnp.int32).at[dest].set(jnp.arange(PAIRS, dtype=jnp.int32))
    return jnp.take(rotated, source, axis=0)
```

```python
import functools

import jax
import jax.numpy as jnp
from jax import lax
from jax.experimental import pallas as pl
from jax.experimental.pallas import tpu as pltpu
from jax.sharding import PartitionSpec as P

MESH = pl.DeviceIdType.MESH
SPLIT = 2
ROUNDS = (4, 5, 6, 7, 8)
RIGHT, LEFT, CROSS = 0, 1, 2


def with_halo(block, sides, width):
    for axis, dim in sides:
        count = lax.axis_size(axis)
        forward = [(i, i + 1) for i in range(count - 1)]
        forward.append((count - 1, 0))
        backward = [(target, source) for source, target in forward]
        low = lax.ppermute(
            lax.slice_in_dim(block, block.shape[dim] - width, None, axis=dim), axis, forward
        )
        high = lax.ppermute(lax.slice_in_dim(block, 0, width, axis=dim), axis, backward)
        block = jnp.concatenate([low, block, high], axis=dim)
    return block


def plan_kernel(
    devices, per, split, limit, dest_ref, sched_ref, final_ref, count_ref, node, slot, goal, order, used
):
    items = devices * per * split

    def clear_sched(i, _):
        sched_ref[i] = 0
        return 0

    lax.fori_loop(0, limit * devices * 3, clear_sched, 0)

    def clear_used(i, _):
        used[i] = 0
        return 0

    lax.fori_loop(0, devices * 3, clear_used, 0)

    def init(i, _):
        pair = i // split
        node[i] = pair // per
        slot[i] = i % (per * split)
        goal[i] = dest_ref[pair] // per
        return 0

    lax.fori_loop(0, items, init, 0)

    def rank(step, at):
        far = devices // 2 - 1 - step

        def visit(i, at):
            here, there = node[i], goal[i]
            hit = (jnp.abs(here // 2 - there // 2) == far) & (here != there)

            @pl.when(hit)
            def _():
                order[at] = i

            return at + hit.astype(jnp.int32)

        return lax.fori_loop(0, items, visit, at)

    moving = lax.fori_loop(0, devices // 2, rank, jnp.int32(0))

    def go_on(carry):
        step, left = carry
        return (left > 0) & (step < limit)

    def one_round(carry):
        step, _ = carry

        def visit(k, left):
            i = order[k]
            here, there = node[i], goal[i]
            z, tz = here // 2, there // 2
            x, tx = here % 2, there % 2
            along = z != tz
            up = tz > z
            key = here * 3 + jnp.where(up, RIGHT, LEFT)
            take = along & (used[key] != step + 1)
            side = here * 3 + CROSS
            swap = jnp.logical_not(take) & (x != tx) & (used[side] != step + 1)
            pick = jnp.where(take, key, side)
            moved = jnp.where(take, here + jnp.where(up, 2, -2), here + 1 - 2 * x)

            @pl.when(take | swap)
            def _():
                used[pick] = step + 1
                sched_ref[step * devices * 3 + pick] = slot[i]
                node[i] = moved
                slot[i] = per * split + 3 * step + (pick - here * 3)

            now = jnp.where(take | swap, moved, here)
            return left + (now != there).astype(jnp.int32)

        return step + 1, lax.fori_loop(0, moving, visit, jnp.int32(0))

    step, left = lax.while_loop(go_on, one_round, (jnp.int32(0), moving))
    count_ref[0] = jnp.where(left > 0, limit + 1, step)

    def finish(i, _):
        there = dest_ref[i // split]
        final_ref[there * split + i % split] = slot[i]
        return 0

    lax.fori_loop(0, items, finish, 0)


def plan(dest, devices, per, split, limit):
    items = devices * per * split
    smem = pl.BlockSpec(memory_space=pltpu.SMEM)
    return pl.pallas_call(
        functools.partial(plan_kernel, devices, per, split, limit),
        out_shape=(
            jax.ShapeDtypeStruct((limit * devices * 3,), jnp.int32),
            jax.ShapeDtypeStruct((items,), jnp.int32),
            jax.ShapeDtypeStruct((1,), jnp.int32),
        ),
        in_specs=[smem],
        out_specs=(smem, smem, smem),
        scratch_shapes=[pltpu.SMEM((items,), jnp.int32)] * 4
        + [pltpu.SMEM((devices * 3,), jnp.int32)],
    )(dest)


def route_kernel(rounds, devices, per, split, sched_ref, final_ref, blocks_ref, out_ref, *rest):
    colours = blocks_ref.shape[1]
    own = rest[:colours]
    recv = rest[colours : colours + rounds * colours]
    stage, own_sem, send_sem, recv_sem = rest[colours + rounds * colours :]
    held = per * split
    rows = blocks_ref.shape[3]
    step_rows = 48
    me = lax.axis_index("ops")
    z, x = me // 2, me % 2
    has = (z < devices // 2 - 1, z > 0, x >= 0)
    back = (has[LEFT], has[RIGHT], has[CROSS])
    to = (me + 2, me - 2, me + 1 - 2 * x)
    peers = 1 + has[RIGHT].astype(jnp.int32) + has[LEFT].astype(jnp.int32)

    barrier = pltpu.get_barrier_semaphore()
    for d in range(3):

        @pl.when(has[d])
        def _():
            pl.semaphore_signal(barrier, inc=1, device_id={"ops": to[d]}, device_id_type=MESH)

    loads = [
        pltpu.make_async_copy(
            blocks_ref.at[p, k], own[k].at[pl.ds(p * split, split)], own_sem.at[p, k]
        )
        for k in range(colours)
        for p in range(per)
    ]
    for load in loads:
        load.start()
    for load in loads:
        load.wait()
    pl.semaphore_wait(barrier, peers)

    def copy(r, k, d):
        return pltpu.make_async_remote_copy(
            src_ref=stage.at[k, d],
            dst_ref=recv[r * colours + k].at[d],
            send_sem=send_sem.at[r, k, d],
            recv_sem=recv_sem.at[r, k, d],
            device_id={"ops": to[d]},
            device_id_type=MESH,
        )

    def select(k, upto, index, at):
        value = own[k][jnp.clip(index, 0, held - 1), pl.ds(at, step_rows), :]
        for j in range(upto):
            base = held + 3 * j
            other = recv[j * colours + k][jnp.clip(index - base, 0, 2), pl.ds(at, step_rows), :]
            value = jnp.where(index >= base, other, value)
        return value

    def finish(r, k):
        for d in range(3):

            @pl.when(has[d])
            def _():
                copy(r, k, d).wait_send()

            @pl.when(back[d])
            def _():
                copy(r, k, d).wait_recv()

    for r in range(rounds):
        for k in range(colours):
            if r > 0:
                finish(r - 1, k)
            for d in range(3):
                index = sched_ref[r * devices * 3 + me * 3 + d]

                @pl.loop(0, rows // step_rows)
                def _(c):
                    at = pl.multiple_of(c * step_rows, step_rows)
                    stage[k, d, pl.ds(at, step_rows), :] = select(k, r, index, at)

                @pl.when(has[d])
                def _():
                    copy(r, k, d).start()

    for k in range(colours):
        finish(rounds - 1, k)
        for q in range(per):
            for h in range(split):
                index = final_ref[me * held + q * split + h]

                @pl.loop(0, rows // step_rows)
                def _(c):
                    at = pl.multiple_of(c * step_rows, step_rows)
                    out_ref[q, k, h, pl.ds(at, step_rows), :] = select(k, rounds, index, at)


def route(rounds, devices, split, sched, final, operators):
    per, colours, width, columns = operators.shape
    rows = width // split
    dtype = operators.dtype
    smem = pl.BlockSpec(memory_space=pltpu.SMEM)
    out = pl.pallas_call(
        functools.partial(route_kernel, rounds, devices, per, split),
        out_shape=jax.ShapeDtypeStruct((per, colours, split, rows, columns), dtype),
        in_specs=[smem, smem, pl.BlockSpec(memory_space=pl.ANY)],
        out_specs=pl.BlockSpec(memory_space=pltpu.VMEM),
        scratch_shapes=[pltpu.VMEM((per * split, rows, columns), dtype)] * colours
        + [pltpu.VMEM((3, rows, columns), dtype)] * (rounds * colours)
        + [
            pltpu.VMEM((colours, 3, rows, columns), dtype),
            pltpu.SemaphoreType.DMA((per, colours)),
            pltpu.SemaphoreType.DMA((rounds, colours, 3)),
            pltpu.SemaphoreType.DMA((rounds, colours, 3)),
        ],
        compiler_params=pltpu.CompilerParams(
            collective_id=rounds, has_side_effects=True, vmem_limit_bytes=60 * 1024 * 1024
        ),
    )(sched, final, operators.reshape(per, colours, split, rows, columns))
    return out.reshape(operators.shape)


def exchange(operators, source):
    pair_dev, sector_dev, width = operators.shape[:3]
    ops_count = lax.axis_size("ops")
    strip = width // ops_count
    split = operators.reshape(pair_dev, sector_dev, ops_count, strip, operators.shape[3])
    spread = lax.all_to_all(split, "ops", split_axis=2, concat_axis=0, tiled=True)
    ordered = jnp.take(spread, source, axis=0)
    returned = lax.all_to_all(ordered, "ops", split_axis=0, concat_axis=2, tiled=True)
    return returned.reshape(operators.shape)


def reassign(operators, dest, source):
    devices = lax.axis_size("ops")
    per, _, width, _ = operators.shape
    limit = max(ROUNDS)
    if devices > 2 * ROUNDS[0] or devices % 2 or width % (SPLIT * 48):
        return exchange(operators, source)
    sched, final, count = plan(dest, devices, per, SPLIT, limit)
    index = sum((count[0] > r).astype(jnp.int32) for r in ROUNDS)
    branches = [functools.partial(route, r, devices, SPLIT) for r in ROUNDS]
    branches.append(lambda sched, final, operators: exchange(operators, source))
    return lax.switch(index, branches, sched, final, operators)


def body(operators, basis, shift, dest, sector_sizes):
    pair_dev = operators.shape[0]
    sector_dev = operators.shape[1]
    width = operators.shape[3]
    total_sectors = sector_dev * lax.axis_size("sec")
    sector_pos = lax.axis_index("sec")
    ops_pos = lax.axis_index("ops")
    nearby = with_halo(basis, (("sec", 0),), 1)
    near_ids = (
        sector_pos * sector_dev - 1 + jnp.arange(sector_dev + 2, dtype=jnp.int32)
    ) % total_sectors
    own_local = jnp.arange(sector_dev, dtype=jnp.int32) + 1
    columns = jnp.arange(width, dtype=jnp.int32)
    near_sizes = jnp.take(sector_sizes, near_ids)
    kept = columns[None, :] < near_sizes[:, None]
    kept_near = jnp.where(kept[:, None, :], nearby, jnp.zeros_like(nearby))
    own_basis = lax.slice_in_dim(kept_near, 1, 1 + sector_dev, axis=0)
    source = jnp.argsort(dest, stable=True)
    mine = lax.dynamic_slice_in_dim(source, ops_pos * pair_dev, pair_dev)
    offsets = jnp.take(shift, mine)
    blocks = reassign(operators, dest, source)
    target_local = own_local[None, :] + offsets[:, None]
    half = jnp.einsum(
        "psab,sbc->psac", blocks, own_basis, preferred_element_type=jnp.float32
    ).astype(jnp.bfloat16)
    targets = jnp.take(kept_near, target_local.reshape(-1), axis=0)
    targets = targets.reshape(blocks.shape[0], sector_dev, width, width)
    return jnp.einsum("psba,psbc->psac", targets, half, preferred_element_type=jnp.float32).astype(
        jnp.bfloat16
    )


def solution(mesh):
    return jax.shard_map(
        body,
        mesh=mesh,
        in_specs=(P("ops", "sec", None, None), P("sec", None, None), P(), P(), P()),
        out_specs=P("ops", "sec", None, None),
        check_vma=False,
    )
```

```python
import functools

import jax
import jax.numpy as jnp
from jax import lax
from jax.experimental import pallas as pl
from jax.experimental.pallas import tpu as pltpu
from jax.sharding import PartitionSpec as P

MESH = pl.DeviceIdType.MESH
SPLIT = 3
ROUNDS = (6, 7, 8, 9, 10, 11)
STEP_ROWS = 64
RIGHT, LEFT, CROSS = 0, 1, 2


def plan_kernel(
    devices, per, split, limit, dest_ref, shift_ref,
    sched_ref, final_ref, count_ref, offset_ref,
    node, slot, goal, order, used, load,
):
    held = per * split
    items = devices * held

    def clear(ref, size):
        def one(i, _):
            ref[i] = 0
            return 0

        lax.fori_loop(0, size, one, 0, unroll=8)

    clear(sched_ref, limit * devices * 3)
    clear(used, devices * 3)
    clear(load, devices * 2)

    def rank(step, at):
        far = devices // 2 - 1 - step

        def visit(pair, at):
            here, there = lax.div(pair, per), lax.div(dest_ref[pair], per)
            gap = lax.shift_right_logical(there, 1) - lax.shift_right_logical(here, 1)
            hit = (jnp.abs(gap) == far) & (here != there)

            @pl.when(hit)
            def _():
                for h in range(split):
                    i = pair * split + h
                    order[at + h] = i
                    node[i] = here
                    goal[i] = there
                    slot[i] = lax.rem(pair, per) * split + h

            @pl.when(hit & (gap != 0))
            def _():
                lane = here * 2 + jnp.where(gap > 0, RIGHT, LEFT)
                load[lane] = load[lane] + split

            return at + jnp.where(hit, split, 0)

        return lax.fori_loop(0, devices * per, visit, at)

    def stay(pair, _):
        there = dest_ref[pair]
        offset_ref[there] = shift_ref[pair]
        for h in range(split):
            slot[pair * split + h] = lax.rem(pair, per) * split + h
        return 0

    lax.fori_loop(0, devices * per, stay, 0)
    moving = lax.fori_loop(0, devices // 2, rank, jnp.int32(0))

    def go_on(carry):
        step, left = carry
        return (left > 0) & (step < limit)

    def one_round(carry):
        step, active = carry

        def visit(k, left):
            i = order[k]
            here, there = node[i], goal[i]
            gap = lax.shift_right_logical(there, 1) - lax.shift_right_logical(here, 1)
            along = gap != 0
            way = jnp.where(gap > 0, RIGHT, LEFT)
            beside = here ^ 1
            aside = (here & 1) != (there & 1)
            key, side = here * 3 + way, here * 3 + CROSS
            lane, other = here * 2 + way, beside * 2 + way
            margin = load[lane] - load[other]
            take = along & (used[key] != step + 1)
            fits = jnp.where(along, margin >= jnp.where(aside, 0, 2), aside)
            swap = jnp.logical_not(take) & fits & (used[side] != step + 1)
            go = take | swap
            pick = jnp.where(take, key, side)
            moved = jnp.where(take, here + 2 - 4 * way, beside)
            now = jnp.where(go, moved, here)

            @pl.when(go)
            def _():
                used[pick] = step + 1
                sched_ref[step * devices * 3 + pick] = slot[i]
                node[i] = moved
                slot[i] = held + 3 * step + (pick - here * 3)

            @pl.when(go & along)
            def _():
                ahead = moved * 2 + way
                further = lax.shift_right_logical(moved, 1) != lax.shift_right_logical(there, 1)
                load[lane] = load[lane] - 1
                load[ahead] = load[ahead] + further.astype(jnp.int32)

            order[left] = i
            return left + (now != there).astype(jnp.int32)

        return step + 1, lax.fori_loop(0, active, visit, jnp.int32(0))

    step, left = lax.while_loop(go_on, one_round, (jnp.int32(0), moving))
    count_ref[0] = jnp.where(left > 0, limit + 1, step)

    def finish(pair, _):
        there = dest_ref[pair]
        for h in range(split):
            final_ref[there * split + h] = slot[pair * split + h]
        return 0

    lax.fori_loop(0, devices * per, finish, 0)


def plan(dest, shift, devices, per, split, limit):
    items = devices * per * split
    smem = pl.BlockSpec(memory_space=pltpu.SMEM)
    return pl.pallas_call(
        functools.partial(plan_kernel, devices, per, split, limit),
        out_shape=(
            jax.ShapeDtypeStruct((limit * devices * 3,), jnp.int32),
            jax.ShapeDtypeStruct((items,), jnp.int32),
            jax.ShapeDtypeStruct((1,), jnp.int32),
            jax.ShapeDtypeStruct((devices * per,), jnp.int32),
        ),
        in_specs=[smem, smem],
        out_specs=(smem, smem, smem, smem),
        scratch_shapes=[pltpu.SMEM((items,), jnp.int32)] * 4
        + [pltpu.SMEM((devices * 3,), jnp.int32), pltpu.SMEM((devices * 2,), jnp.int32)],
    )(dest, shift)


def route_kernel(rounds, devices, per, split, sched_ref, final_ref, blocks_ref, out_ref, *rest):
    colours = blocks_ref.shape[1]
    own = rest[:colours]
    recv = rest[colours : colours + rounds * colours]
    stage, own_sem, send_sem, recv_sem = rest[colours + rounds * colours :]
    held = per * split
    rows = blocks_ref.shape[3]
    step_rows = STEP_ROWS
    me = lax.axis_index("ops")
    z, x = me // 2, me % 2
    has = (z < devices // 2 - 1, z > 0, x >= 0)
    back = (has[LEFT], has[RIGHT], has[CROSS])
    to = (me + 2, me - 2, me + 1 - 2 * x)
    peers = 1 + has[RIGHT].astype(jnp.int32) + has[LEFT].astype(jnp.int32)

    barrier = pltpu.get_barrier_semaphore()
    for d in range(3):

        @pl.when(has[d])
        def _():
            pl.semaphore_signal(barrier, inc=1, device_id={"ops": to[d]}, device_id_type=MESH)

    loads = [
        pltpu.make_async_copy(
            blocks_ref.at[p, k], own[k].at[pl.ds(p * split, split)], own_sem.at[p, k]
        )
        for k in range(colours)
        for p in range(per)
    ]
    for load in loads:
        load.start()
    for load in loads:
        load.wait()
    pl.semaphore_wait(barrier, peers)

    def copy(r, k, d):
        return pltpu.make_async_remote_copy(
            src_ref=stage.at[k, d],
            dst_ref=recv[r * colours + k].at[d],
            send_sem=send_sem.at[r, k, d],
            recv_sem=recv_sem.at[r, k, d],
            device_id={"ops": to[d]},
            device_id_type=MESH,
        )

    def select(k, upto, index, at):
        value = own[k][jnp.clip(index, 0, held - 1), pl.ds(at, step_rows), :]
        for j in range(upto):
            base = held + 3 * j
            other = recv[j * colours + k][jnp.clip(index - base, 0, 2), pl.ds(at, step_rows), :]
            value = jnp.where(index >= base, other, value)
        return value

    def finish(r, k):
        for d in range(3):

            @pl.when(has[d])
            def _():
                copy(r, k, d).wait_send()

            @pl.when(back[d])
            def _():
                copy(r, k, d).wait_recv()

    for r in range(rounds):
        for k in range(colours):
            if r > 0:
                finish(r - 1, k)
            for d in range(3):
                index = sched_ref[r * devices * 3 + me * 3 + d]

                @pl.loop(0, rows // step_rows)
                def _(c):
                    at = pl.multiple_of(c * step_rows, step_rows)
                    stage[k, d, pl.ds(at, step_rows), :] = select(k, r, index, at)

                @pl.when(has[d])
                def _():
                    copy(r, k, d).start()

    for k in range(colours):
        finish(rounds - 1, k)
        for q in range(per):
            for h in range(split):
                index = final_ref[me * held + q * split + h]

                @pl.loop(0, rows // step_rows)
                def _(c):
                    at = pl.multiple_of(c * step_rows, step_rows)
                    out_ref[q, k, h, pl.ds(at, step_rows), :] = select(k, rounds, index, at)


def route(rounds, devices, split, sched, final, operators):
    per, colours, width, columns = operators.shape
    rows = width // split
    dtype = operators.dtype
    smem = pl.BlockSpec(memory_space=pltpu.SMEM)
    out = pl.pallas_call(
        functools.partial(route_kernel, rounds, devices, per, split),
        out_shape=jax.ShapeDtypeStruct((per, colours, split, rows, columns), dtype),
        in_specs=[smem, smem, pl.BlockSpec(memory_space=pl.ANY)],
        out_specs=pl.BlockSpec(memory_space=pltpu.VMEM),
        scratch_shapes=[pltpu.VMEM((per * split, rows, columns), dtype)] * colours
        + [pltpu.VMEM((3, rows, columns), dtype)] * (rounds * colours)
        + [
            pltpu.VMEM((colours, 3, rows, columns), dtype),
            pltpu.SemaphoreType.DMA((per, colours)),
            pltpu.SemaphoreType.DMA((rounds, colours, 3)),
            pltpu.SemaphoreType.DMA((rounds, colours, 3)),
        ],
        compiler_params=pltpu.CompilerParams(
            collective_id=rounds, has_side_effects=True, vmem_limit_bytes=60 * 1024 * 1024
        ),
    )(sched, final, operators.reshape(per, colours, split, rows, columns))
    return out.reshape(operators.shape)


def exchange(operators, dest):
    pair_dev, sector_dev, width = operators.shape[:3]
    ops_count = lax.axis_size("ops")
    strip = width // ops_count
    source = jnp.argsort(dest, stable=True)
    split = operators.reshape(pair_dev, sector_dev, ops_count, strip, operators.shape[3])
    spread = lax.all_to_all(split, "ops", split_axis=2, concat_axis=0, tiled=True)
    ordered = jnp.take(spread, source, axis=0)
    returned = lax.all_to_all(ordered, "ops", split_axis=0, concat_axis=2, tiled=True)
    return returned.reshape(operators.shape)


def reassign(operators, dest, shift):
    devices = lax.axis_size("ops")
    per, _, width, _ = operators.shape
    limit = max(ROUNDS)
    if devices > 2 * ROUNDS[0] or devices % 2 or width % (SPLIT * STEP_ROWS):
        offsets = jnp.take(shift, jnp.argsort(dest, stable=True))
        return exchange(operators, dest), offsets
    sched, final, count, offsets = plan(dest, shift, devices, per, SPLIT, limit)
    index = sum((count[0] > r).astype(jnp.int32) for r in ROUNDS)
    branches = [functools.partial(route, r, devices, SPLIT) for r in ROUNDS]
    branches.append(lambda sched, final, operators: exchange(operators, dest))
    return lax.switch(index, branches, sched, final, operators), offsets


def rotate_kernel(
    total, offset_ref, sizes_ref, low_ref, basis_ref, high_ref, block_ref, out_ref, near, sem
):
    per, sectors = pl.num_programs(0), pl.num_programs(1)
    p, s = pl.program_id(0), pl.program_id(1)
    count = basis_ref.shape[0]

    @pl.when((p == 0) & (s == 0))
    def _():
        copies = [
            pltpu.make_async_copy(low_ref, near.at[pl.ds(0, 1)], sem.at[0]),
            pltpu.make_async_copy(basis_ref, near.at[pl.ds(1, count)], sem.at[1]),
            pltpu.make_async_copy(high_ref, near.at[pl.ds(count + 1, 1)], sem.at[2]),
        ]
        for copy in copies:
            copy.start()
        for copy in copies:
            copy.wait()

    offset = offset_ref[lax.axis_index("ops") * per + p]
    sector = lax.axis_index("sec") * sectors + s
    kept_columns = sizes_ref[sector]
    kept_rows = sizes_ref[lax.rem(sector + offset + total, total)]
    half = jnp.dot(block_ref[0, 0], near[1 + s], preferred_element_type=jnp.float32)
    half = half.astype(block_ref.dtype)
    full = lax.dot_general(
        near[1 + s + offset], half, (((0,), (0,)), ((), ())), preferred_element_type=jnp.float32
    )
    row = lax.broadcasted_iota(jnp.int32, full.shape, 0)
    column = lax.broadcasted_iota(jnp.int32, full.shape, 1)
    full = jnp.where((row < kept_rows) & (column < kept_columns), full, 0.0)
    out_ref[0, 0] = full.astype(out_ref.dtype)


def rotate(blocks, low, basis, high, offsets, sector_sizes, total):
    per, sectors, width, columns = blocks.shape
    smem = pl.BlockSpec(memory_space=pltpu.SMEM)
    hbm = pl.BlockSpec(memory_space=pl.ANY)
    one = pl.BlockSpec((1, 1, width, columns), lambda p, s: (p, s, 0, 0))
    return pl.pallas_call(
        functools.partial(rotate_kernel, total),
        grid=(per, sectors),
        out_shape=jax.ShapeDtypeStruct(blocks.shape, blocks.dtype),
        in_specs=[smem, smem, hbm, hbm, hbm, one],
        out_specs=one,
        scratch_shapes=[
            pltpu.VMEM((sectors + 2, width, columns), blocks.dtype),
            pltpu.SemaphoreType.DMA((3,)),
        ],
        cost_estimate=pl.CostEstimate(
            flops=4 * per * sectors * width**3, bytes_accessed=4 * blocks.size, transcendentals=0
        ),
    )(offsets, sector_sizes, low, basis, high, blocks)


def body(operators, basis, shift, dest, sector_sizes):
    count = lax.axis_size("sec")
    forward = [(i, (i + 1) % count) for i in range(count)]
    backward = [(target, source) for source, target in forward]
    low = lax.ppermute(basis[-1:], "sec", forward)
    high = lax.ppermute(basis[:1], "sec", backward)
    blocks, offsets = reassign(operators, dest, shift)
    total = basis.shape[0] * count
    return rotate(blocks, low, basis, high, offsets, sector_sizes, total)


def solution(mesh):
    return jax.shard_map(
        body,
        mesh=mesh,
        in_specs=(P("ops", "sec", None, None), P("sec", None, None), P(), P(), P()),
        out_specs=P("ops", "sec", None, None),
        check_vma=False,
    )
```

```python
import functools

import jax
import jax.numpy as jnp
from jax import lax
from jax.experimental import pallas as pl
from jax.experimental.pallas import tpu as pltpu
from jax.sharding import PartitionSpec as P

MESH = pl.DeviceIdType.MESH
SPLIT = 3
ROUNDS = (6, 7, 8, 9, 10, 11)
STEP_ROWS = 64
RIGHT, LEFT, CROSS = 0, 1, 2


def plan_kernel(
    devices, per, split, limit, dest_ref, shift_ref,
    sched_ref, final_ref, count_ref, offset_ref,
    node, slot, goal, order, used, load,
):
    held = per * split
    items = devices * held

    def clear(ref, size):
        def one(i, _):
            ref[i] = 0
            return 0

        lax.fori_loop(0, size, one, 0, unroll=8)

    clear(sched_ref, limit * devices * 3 + 1)
    clear(used, devices * 3 + 1)
    clear(load, devices * 2)

    def rank(step, at):
        far = devices // 2 - 1 - step

        def visit(pair, at):
            here, there = lax.div(pair, per), lax.div(dest_ref[pair], per)
            gap = lax.shift_right_logical(there, 1) - lax.shift_right_logical(here, 1)
            hit = (jnp.abs(gap) == far) & (here != there)

            @pl.when(hit)
            def _():
                for h in range(split):
                    i = pair * split + h
                    order[at + h] = i
                    node[i] = here
                    goal[i] = there
                    slot[i] = lax.rem(pair, per) * split + h

            @pl.when(hit & (gap != 0))
            def _():
                lane = here * 2 + jnp.where(gap > 0, RIGHT, LEFT)
                load[lane] = load[lane] + split

            return at + jnp.where(hit, split, 0)

        return lax.fori_loop(0, devices * per, visit, at)

    def stay(pair, _):
        there = dest_ref[pair]
        offset_ref[there] = shift_ref[pair]
        for h in range(split):
            slot[pair * split + h] = lax.rem(pair, per) * split + h
        return 0

    lax.fori_loop(0, devices * per, stay, 0)
    moving = lax.fori_loop(0, devices // 2, rank, jnp.int32(0))

    def go_on(carry):
        step, left = carry
        return (left > 0) & (step < limit)

    def one_round(carry):
        step, active = carry

        def visit(k, left):
            i = order[k]
            here, there = node[i], goal[i]
            gap = lax.shift_right_logical(there, 1) - lax.shift_right_logical(here, 1)
            along = gap != 0
            way = jnp.where(gap > 0, RIGHT, LEFT)
            beside = here ^ 1
            aside = (here & 1) != (there & 1)
            key, side = here * 3 + way, here * 3 + CROSS
            lane, other = here * 2 + way, beside * 2 + way
            margin = load[lane] - load[other]
            take = along & (used[key] != step + 1)
            fits = jnp.where(along, margin >= jnp.where(aside, 0, 2), aside)
            swap = jnp.logical_not(take) & fits & (used[side] != step + 1)
            go = take | swap
            pick = jnp.where(take, key, side)
            moved = jnp.where(take, here + 2 - 4 * way, beside)
            now = jnp.where(go, moved, here)

            old = slot[i]
            spot = step * devices * 3 + pick
            used[jnp.where(go, pick, devices * 3)] = step + 1
            sched_ref[jnp.where(go, spot, limit * devices * 3)] = old
            node[i] = now
            slot[i] = jnp.where(go, held + 3 * step + (pick - here * 3), old)
            ahead = now * 2 + way
            gone = go & along
            further = lax.shift_right_logical(now, 1) != lax.shift_right_logical(there, 1)
            load[lane] = load[lane] - gone.astype(jnp.int32)
            load[ahead] = load[ahead] + (gone & further).astype(jnp.int32)
            order[left] = i
            return left + (now != there).astype(jnp.int32)

        return step + 1, lax.fori_loop(0, active, visit, jnp.int32(0))

    step, left = lax.while_loop(go_on, one_round, (jnp.int32(0), moving))
    total = jnp.where(left > 0, limit + 1, step)
    count_ref[0] = sum((total > r).astype(jnp.int32) for r in ROUNDS)

    def finish(pair, _):
        there = dest_ref[pair]
        for h in range(split):
            final_ref[there * split + h] = slot[pair * split + h]
        return 0

    lax.fori_loop(0, devices * per, finish, 0)


def plan(dest, shift, devices, per, split, limit):
    items = devices * per * split
    smem = pl.BlockSpec(memory_space=pltpu.SMEM)
    return pl.pallas_call(
        functools.partial(plan_kernel, devices, per, split, limit),
        out_shape=(
            jax.ShapeDtypeStruct((limit * devices * 3 + 1,), jnp.int32),
            jax.ShapeDtypeStruct((items,), jnp.int32),
            jax.ShapeDtypeStruct((1,), jnp.int32),
            jax.ShapeDtypeStruct((devices * per,), jnp.int32),
        ),
        in_specs=[smem, smem],
        out_specs=(smem, smem, smem, smem),
        scratch_shapes=[pltpu.SMEM((items,), jnp.int32)] * 4
        + [pltpu.SMEM((devices * 3 + 1,), jnp.int32), pltpu.SMEM((devices * 2,), jnp.int32)],
    )(dest, shift)


def route_kernel(rounds, devices, per, split, sched_ref, final_ref, blocks_ref, basis_ref, out_ref, low_ref, high_ref, *rest):
    colours = blocks_ref.shape[1]
    own = rest[:colours]
    recv = rest[colours : colours + rounds * colours]
    stage, done, own_sem, out_sem, near_sem, send_sem, recv_sem = rest[colours + rounds * colours :]
    held = per * split
    rows = blocks_ref.shape[3]
    step_rows = STEP_ROWS
    me = lax.axis_index("ops")
    z, x = me // 2, me % 2
    has = (z < devices // 2 - 1, z > 0, x >= 0)
    back = (has[LEFT], has[RIGHT], has[CROSS])
    to = (me + 2, me - 2, me + 1 - 2 * x)
    sectors = lax.axis_size("sec")
    at_sec = lax.axis_index("sec")
    after = lax.rem(at_sec + 1, sectors)
    before = lax.rem(at_sec + sectors - 1, sectors)
    last = basis_ref.shape[0] - 1
    halo = [
        pltpu.make_async_remote_copy(
            src_ref=basis_ref.at[pl.ds(start, 1)],
            dst_ref=ref,
            send_sem=near_sem.at[0, e],
            recv_sem=near_sem.at[1, e],
            device_id={"sec": peer},
            device_id_type=MESH,
        )
        for e, (start, ref, peer) in enumerate(((last, low_ref, after), (0, high_ref, before)))
    ]
    peers = 3 + has[RIGHT].astype(jnp.int32) + has[LEFT].astype(jnp.int32)

    barrier = pltpu.get_barrier_semaphore()
    for d in range(3):

        @pl.when(has[d])
        def _():
            pl.semaphore_signal(barrier, inc=1, device_id={"ops": to[d]}, device_id_type=MESH)

    for peer in (after, before):
        pl.semaphore_signal(barrier, inc=1, device_id={"sec": peer}, device_id_type=MESH)

    loads = [
        pltpu.make_async_copy(
            blocks_ref.at[p, k], own[k].at[pl.ds(p * split, split)], own_sem.at[p, k]
        )
        for k in range(colours)
        for p in range(per)
    ]
    for load in loads:
        load.start()
    for load in loads:
        load.wait()
    pl.semaphore_wait(barrier, peers)
    for one in halo:
        one.start()

    def copy(r, k, d):
        return pltpu.make_async_remote_copy(
            src_ref=stage.at[k, d],
            dst_ref=recv[r * colours + k].at[d],
            send_sem=send_sem.at[r, k, d],
            recv_sem=recv_sem.at[r, k, d],
            device_id={"ops": to[d]},
            device_id_type=MESH,
        )

    def select(k, upto, index, at):
        value = own[k][jnp.clip(index, 0, held - 1), pl.ds(at, step_rows), :]
        for j in range(upto):
            base = held + 3 * j
            other = recv[j * colours + k][jnp.clip(index - base, 0, 2), pl.ds(at, step_rows), :]
            value = jnp.where(index >= base, other, value)
        return value

    def finish(r, k):
        for d in range(3):

            @pl.when(has[d])
            def _():
                copy(r, k, d).wait_send()

            @pl.when(back[d])
            def _():
                copy(r, k, d).wait_recv()

    for r in range(rounds):
        for k in range(colours):
            if r > 0:
                finish(r - 1, k)
            for d in range(3):
                index = sched_ref[r * devices * 3 + me * 3 + d]

                @pl.loop(0, rows // step_rows)
                def _(c):
                    at = pl.multiple_of(c * step_rows, step_rows)
                    stage[k, d, pl.ds(at, step_rows), :] = select(k, r, index, at)

                @pl.when(has[d])
                def _():
                    copy(r, k, d).start()

    copies = []
    for k in range(colours):
        finish(rounds - 1, k)
        for q in range(per):
            for h in range(split):
                index = final_ref[me * held + q * split + h]

                @pl.loop(0, rows // step_rows)
                def _(c):
                    at = pl.multiple_of(c * step_rows, step_rows)
                    done[k, q, h, pl.ds(at, step_rows), :] = select(k, rounds, index, at)

            copies.append(pltpu.make_async_copy(done.at[k, q], out_ref.at[q, k], out_sem.at[q, k]))
            copies[-1].start()
    for one in copies + halo:
        one.wait()


def route(rounds, devices, split, sched, final, operators, basis):
    per, colours, width, columns = operators.shape
    rows = width // split
    dtype = operators.dtype
    smem = pl.BlockSpec(memory_space=pltpu.SMEM)
    hbm = pl.BlockSpec(memory_space=pl.ANY)
    edge = jax.ShapeDtypeStruct((1,) + basis.shape[1:], basis.dtype)
    out, low, high = pl.pallas_call(
        functools.partial(route_kernel, rounds, devices, per, split),
        out_shape=(jax.ShapeDtypeStruct((per, colours, split, rows, columns), dtype), edge, edge),
        in_specs=[smem, smem, hbm, hbm],
        out_specs=(hbm, hbm, hbm),
        scratch_shapes=[pltpu.VMEM((per * split, rows, columns), dtype)] * colours
        + [pltpu.VMEM((3, rows, columns), dtype)] * (rounds * colours)
        + [
            pltpu.VMEM((colours, 3, rows, columns), dtype),
            pltpu.VMEM((colours, per, split, rows, columns), dtype),
            pltpu.SemaphoreType.DMA((per, colours)),
            pltpu.SemaphoreType.DMA((per, colours)),
            pltpu.SemaphoreType.DMA((2, 2)),
            pltpu.SemaphoreType.DMA((rounds, colours, 3)),
            pltpu.SemaphoreType.DMA((rounds, colours, 3)),
        ],
        compiler_params=pltpu.CompilerParams(
            collective_id=rounds, has_side_effects=True, vmem_limit_bytes=60 * 1024 * 1024
        ),
    )(sched, final, operators.reshape(per, colours, split, rows, columns), basis)
    return out.reshape(operators.shape), low, high


def exchange(operators, dest):
    pair_dev, sector_dev, width = operators.shape[:3]
    ops_count = lax.axis_size("ops")
    strip = width // ops_count
    source = jnp.argsort(dest, stable=True)
    split = operators.reshape(pair_dev, sector_dev, ops_count, strip, operators.shape[3])
    spread = lax.all_to_all(split, "ops", split_axis=2, concat_axis=0, tiled=True)
    ordered = jnp.take(spread, source, axis=0)
    returned = lax.all_to_all(ordered, "ops", split_axis=0, concat_axis=2, tiled=True)
    return returned.reshape(operators.shape)


def edges(basis):
    count = lax.axis_size("sec")
    forward = [(i, (i + 1) % count) for i in range(count)]
    backward = [(target, source) for source, target in forward]
    return lax.ppermute(basis[-1:], "sec", forward), lax.ppermute(basis[:1], "sec", backward)


def reassign(operators, basis, dest, shift):
    devices = lax.axis_size("ops")
    per, _, width, _ = operators.shape
    limit = max(ROUNDS)
    if devices > 2 * ROUNDS[0] or devices % 2 or lax.axis_size("sec") < 3 or width % (SPLIT * STEP_ROWS):
        offsets = jnp.take(shift, jnp.argsort(dest, stable=True))
        return (exchange(operators, dest), *edges(basis)), offsets
    sched, final, count, offsets = plan(dest, shift, devices, per, SPLIT, limit)
    branches = [functools.partial(route, r, devices, SPLIT) for r in ROUNDS]
    branches.append(lambda sched, final, operators, basis: (exchange(operators, dest), *edges(basis)))
    return lax.switch(count[0], branches, sched, final, operators, basis), offsets


def rotate_kernel(
    total, offset_ref, sizes_ref, low_ref, basis_ref, high_ref, block_ref, out_ref, near, sem
):
    per, sectors = pl.num_programs(0), pl.num_programs(1)
    p, s = pl.program_id(0), pl.program_id(1)
    count = basis_ref.shape[0]

    @pl.when((p == 0) & (s == 0))
    def _():
        copies = [
            pltpu.make_async_copy(low_ref, near.at[pl.ds(0, 1)], sem.at[0]),
            pltpu.make_async_copy(basis_ref, near.at[pl.ds(1, count)], sem.at[1]),
            pltpu.make_async_copy(high_ref, near.at[pl.ds(count + 1, 1)], sem.at[2]),
        ]
        for copy in copies:
            copy.start()
        for copy in copies:
            copy.wait()

    offset = offset_ref[lax.axis_index("ops") * per + p]
    sector = lax.axis_index("sec") * sectors + s
    kept_columns = sizes_ref[sector]
    kept_rows = sizes_ref[lax.rem(sector + offset + total, total)]
    half = jnp.dot(block_ref[0, 0], near[1 + s], preferred_element_type=jnp.float32)
    half = half.astype(block_ref.dtype)
    full = lax.dot_general(
        near[1 + s + offset], half, (((0,), (0,)), ((), ())), preferred_element_type=jnp.float32
    )
    row = lax.broadcasted_iota(jnp.int32, full.shape, 0)
    column = lax.broadcasted_iota(jnp.int32, full.shape, 1)
    full = jnp.where((row < kept_rows) & (column < kept_columns), full, 0.0)
    out_ref[0, 0] = full.astype(out_ref.dtype)


def rotate(blocks, low, basis, high, offsets, sector_sizes, total):
    per, sectors, width, columns = blocks.shape
    smem = pl.BlockSpec(memory_space=pltpu.SMEM)
    hbm = pl.BlockSpec(memory_space=pl.ANY)
    one = pl.BlockSpec((1, 1, width, columns), lambda p, s: (p, s, 0, 0))
    return pl.pallas_call(
        functools.partial(rotate_kernel, total),
        grid=(per, sectors),
        out_shape=jax.ShapeDtypeStruct(blocks.shape, blocks.dtype),
        in_specs=[smem, smem, hbm, hbm, hbm, one],
        out_specs=one,
        scratch_shapes=[
            pltpu.VMEM((sectors + 2, width, columns), blocks.dtype),
            pltpu.SemaphoreType.DMA((3,)),
        ],
        cost_estimate=pl.CostEstimate(
            flops=4 * per * sectors * width**3, bytes_accessed=4 * blocks.size, transcendentals=0
        ),
    )(offsets, sector_sizes, low, basis, high, blocks)


def body(operators, basis, shift, dest, sector_sizes):
    count = lax.axis_size("sec")
    (blocks, low, high), offsets = reassign(operators, basis, dest, shift)
    total = basis.shape[0] * count
    return rotate(blocks, low, basis, high, offsets, sector_sizes, total)


def solution(mesh):
    return jax.shard_map(
        body,
        mesh=mesh,
        in_specs=(P("ops", "sec", None, None), P("sec", None, None), P(), P(), P()),
        out_specs=P("ops", "sec", None, None),
        check_vma=False,
    )
```
